32 devices in a mesh: fsdp: 8 (over y, x, core), tp: 4 (over z).
Axes of the slice: x: 2, y: 2, z: 4, core: 2. Of those that a mesh axis runs over, the one named last changes fastest.
Arguments:
- layer_inputs: bfloat16 [1, 2048, 3584], P(None, ('fsdp', 'tp')), may hold values from -6 to 6
- out_grad: bfloat16 [2048, 3584], P(('fsdp', 'tp')), may hold values from -6 to 6
- pre_scale: float32 [1, 3584], replicated, may hold values from 0.1 to 1.9
- post_scale: float32 [1, 3584], replicated, may hold values from 0.1 to 1.9
- gate_weight: bfloat16 [1, 3584, 3584], P(None, 'fsdp', 'tp'), may hold values from -0.09375 to 0.09375
- up_weight: bfloat16 [1, 3584, 3584], P(None, 'fsdp', 'tp'), may hold values from -0.09375 to 0.09375
- down_weight: bfloat16 [1, 3584, 3584], P(None, 'tp', 'fsdp'), may hold values from -0.09375 to 0.09375
Outputs:
- input_grad: bfloat16 [2048, 3584], P(('fsdp', 'tp'))
- gate_grad: bfloat16 [1, 3584, 3584], P(None, 'fsdp', 'tp')
- up_grad: bfloat16 [1, 3584, 3584], P(None, 'fsdp', 'tp')
- down_grad: bfloat16 [1, 3584, 3584], P(None, 'tp', 'fsdp')
The draws below stay inside these ranges and needn't reach their ends.
All inputs are finite; a program needn't handle non-finite values.
Results may differ from the reference program's by a relative error of at most 0.02.
Values may be sent and summed in bfloat16 or wider, within the bound.
A program may use at most 128 MiB of HBM per device.

```python
import math
import jax
import jax.numpy as jnp
from jax import lax

D = 3584
LAYERS = 1
FF = 3584
TOKENS = 2048


def block_levels(key, extent, cuts, least, top_value):
    loudness, own = 1.0, jax.random.fold_in(key, 6)
    for dim, shards_of in cuts:
        steps = jnp.exp(jax.random.uniform(jax.random.fold_in(own, dim), (shards_of,), jnp.float32, least / len(cuts), top_value / len(cuts)))
        loudness = loudness * jnp.repeat(steps, extent[dim] // shards_of).reshape([-1 if axis == dim else 1 for axis in range(len(extent))])
    return loudness


def centred(stream_key, dims, deviation, most, pieces=(), dtype=jnp.bfloat16):
    loudness = block_levels(stream_key, dims, pieces, -0.22, 0.18) if pieces else 1.0
    entries = jax.random.normal(stream_key, dims, jnp.float32) * deviation * loudness
    return jnp.minimum(jnp.maximum(entries, -most), most).astype(dtype)


def setup_inputs(seed: int = 0) -> dict:
    keys = jax.random.split(jax.random.key(seed), 8)
    return {
        "layer_inputs": centred(keys[0], (LAYERS, TOKENS, D), 1.0, 6.0, ((1, 32),)),
        "out_grad": centred(keys[1], (TOKENS, D), 1.0, 6.0, ((0, 32),)),
        "pre_scale": jnp.clip(1.0 + 0.18 * jax.random.normal(keys[2], (LAYERS, D), jnp.float32), 0.1, 1.9),
        "post_scale": jnp.clip(1.0 + 0.18 * jax.random.normal(keys[3], (LAYERS, D), jnp.float32), 0.1, 1.9),
        "gate_weight": centred(keys[4], (LAYERS, D, FF), D ** -0.5, 0.09375, ((1, 8), (2, 4))),
        "up_weight": centred(keys[5], (LAYERS, D, FF), D ** -0.5, 0.09375, ((1, 8), (2, 4))),
        "down_weight": centred(keys[6], (LAYERS, FF, D), FF ** -0.5, 0.09375, ((1, 4), (2, 8))),
    }


epsilon = 1e-06

def rms_factor(values):
    return lax.rsqrt(lax.optimization_barrier(jnp.mean(values * values, axis=-1, keepdims=True)) + epsilon)

def norm_back(delta, normed_in, factor):
    return factor * (delta - normed_in * lax.optimization_barrier(jnp.mean(delta * normed_in, axis=-1, keepdims=True)))

def gelu_tanh(values):
    return jax.nn.gelu(values, approximate=True)

def reference(layer_inputs, out_grad, pre_scale, post_scale, gate_weight, up_weight, down_weight):
    grad_scale = 1.0 / math.sqrt(TOKENS)
    carried = out_grad.astype(jnp.float32)
    gate_list = [None] * LAYERS
    up_list = [None] * LAYERS
    down_list = [None] * LAYERS
    for layer_id in reversed(range(LAYERS)):
        layer_in = layer_inputs[layer_id].astype(jnp.float32)
        first_rms = rms_factor(layer_in)
        normed = (layer_in * first_rms * pre_scale[layer_id]).astype(jnp.bfloat16)
        gate_pre = jnp.dot(normed, gate_weight[layer_id], preferred_element_type=jnp.float32)
        up_pre = jnp.dot(normed, up_weight[layer_id], preferred_element_type=jnp.float32)
        active, gelu_back = jax.vjp(gelu_tanh, gate_pre)
        hidden = (active * up_pre).astype(jnp.bfloat16)
        mlp_out = jnp.dot(hidden, down_weight[layer_id], preferred_element_type=jnp.float32)
        mlp_out = lax.optimization_barrier(mlp_out.astype(jnp.bfloat16)).astype(jnp.float32)
        second_rms = rms_factor(mlp_out)
        mlp_grad = norm_back(carried * post_scale[layer_id], mlp_out * second_rms, second_rms).astype(jnp.bfloat16)
        hidden_grad = jnp.dot(mlp_grad, down_weight[layer_id].T, preferred_element_type=jnp.float32)
        gate_delta = gelu_back(hidden_grad * up_pre)[0].astype(jnp.bfloat16)
        up_delta = (hidden_grad * active).astype(jnp.bfloat16)
        gate_list[layer_id] = (jnp.dot(normed.T, gate_delta, preferred_element_type=jnp.float32) * grad_scale).astype(jnp.bfloat16)
        up_list[layer_id] = (jnp.dot(normed.T, up_delta, preferred_element_type=jnp.float32) * grad_scale).astype(jnp.bfloat16)
        down_list[layer_id] = (jnp.dot(hidden.T, mlp_grad, preferred_element_type=jnp.float32) * grad_scale).astype(jnp.bfloat16)
        normed_grad = jnp.dot(gate_delta, gate_weight[layer_id].T, preferred_element_type=jnp.float32)
        normed_grad = normed_grad + jnp.dot(up_delta, up_weight[layer_id].T, preferred_element_type=jnp.float32)
        carried = carried + norm_back(normed_grad * pre_scale[layer_id], layer_in * first_rms, first_rms)
    return (carried.astype(jnp.bfloat16), jnp.stack(gate_list), jnp.stack(up_list), jnp.stack(down_list))
```

```python
import functools
import math

import jax
import jax.numpy as jnp
from jax import lax
from jax.experimental import pallas as pl
from jax.experimental.pallas import tpu as pltpu
from jax.sharding import PartitionSpec as P

epsilon = 1e-06
MESH = pl.DeviceIdType.MESH
VMEM_LIMIT = 60 * 1024 * 1024


def rms_factor(values):
    return lax.rsqrt(jnp.mean(values * values, axis=-1, keepdims=True) + epsilon)


def norm_back(delta, normed_in, factor):
    return factor * (delta - normed_in * jnp.mean(delta * normed_in, axis=-1, keepdims=True))


def gelu_tanh(values):
    return jax.nn.gelu(values, approximate=True)


def place(outer):
    me = lax.axis_index("fsdp")
    return me // 4, (me // 2) % 2, me % 2


def index_of(a, b, c):
    return (a * 2 + b) * 2 + c


def remote(src, dst, send_sem, recv_sem, target):
    return pltpu.make_async_remote_copy(
        src_ref=src,
        dst_ref=dst,
        send_sem=send_sem,
        recv_sem=recv_sem,
        device_id={"fsdp": target},
        device_id_type=MESH,
    )


def greet(outer, a, b, c):
    barrier = pltpu.get_barrier_semaphore()
    targets = [index_of(a, b, 1 - c), index_of(a, 1 - b, c)]
    targets += [index_of((a + j) % outer, b, c) for j in range(1, outer)]
    for target in targets:
        pl.semaphore_signal(barrier, inc=1, device_id={"fsdp": target}, device_id_type=MESH)
    pl.semaphore_wait(barrier, len(targets))


def gather_kernel(outer, count, *refs):
    ins, outs = refs[:count], refs[count : 2 * count]
    bounce, local_sem, recv_sem, link_sem, pair_sem = refs[2 * count :]
    a, b, c = place(outer)
    me = index_of(a, b, c)
    partner = index_of(a, b, 1 - c)
    across = index_of(a, 1 - b, c)
    along = [index_of((a + j) % outer, b, c) for j in range(1, outer)]
    diagonal = [index_of((a + j) % outer, 1 - b, c) for j in range(1, outer)]
    greet(outer, a, b, c)

    def push(w, src, slot, sem, target):
        return remote(src, outs[w].at[slot], sem, recv_sem.at[w, slot], target)

    def arrived(w, slot):
        spot = outs[w].at[slot]
        remote(spot, spot, pair_sem.at[w, 0], recv_sem.at[w, slot], partner).wait_recv()

    sent = []
    for w in range(count):
        own = [push(w, ins[w], me, link_sem.at[w, 0], across)]
        own += [push(w, ins[w], me, link_sem.at[w, 1 + j], t) for j, t in enumerate(along)]
        own.append(push(w, ins[w], me, pair_sem.at[w, 0], partner))
        for copy in own:
            copy.start()
        sent += own
    inward = [pltpu.make_async_copy(ins[w], bounce.at[w], local_sem.at[w]) for w in range(count)]
    outward = [
        pltpu.make_async_copy(bounce.at[w], outs[w].at[me], local_sem.at[w]) for w in range(count)
    ]
    for w in range(count):
        inward[w].start()
    for w in range(count):
        inward[w].wait()
        outward[w].start()
    forwards = []
    for w in range(count):
        arrived(w, across)
        copy = push(w, outs[w].at[across], across, pair_sem.at[w, 1], partner)
        copy.start()
        sent.append(copy)
        for j, target in enumerate(along):
            copy = push(w, outs[w].at[across], across, link_sem.at[w, outer + j], target)
            pl.when(c == 0)(copy.start)
            forwards.append((0, copy))
        for j, slot in enumerate(along):
            arrived(w, slot)
            copy = push(w, outs[w].at[slot], slot, link_sem.at[w, outer + j], across)
            pl.when(c == 1)(copy.start)
            forwards.append((1, copy))
            copy = push(w, outs[w].at[slot], slot, pair_sem.at[w, 2 + j], partner)
            copy.start()
            sent.append(copy)
    for w in range(count):
        for j, slot in enumerate(diagonal):
            arrived(w, slot)
            copy = push(w, outs[w].at[slot], slot, pair_sem.at[w, 1 + outer + j], partner)
            copy.start()
            sent.append(copy)
    for w in range(count):
        for chip in range(2 * outer):
            arrived(w, chip * 2 + 1 - c)
        outward[w].wait()
    for copy in sent:
        copy.wait_send()
    for core, copy in forwards:
        pl.when(c == core)(copy.wait_send)


def gather_blocks(blocks, parts):
    outer, count = parts // 4, len(blocks)
    rows, columns = blocks[0].shape
    dtype = blocks[0].dtype
    size = rows * columns * dtype.itemsize * count
    outs = pl.pallas_call(
        functools.partial(gather_kernel, outer, count),
        out_shape=[jax.ShapeDtypeStruct((parts, rows, columns), dtype)] * count,
        in_specs=[pl.BlockSpec(memory_space=pl.ANY)] * count,
        out_specs=[pl.BlockSpec(memory_space=pl.ANY)] * count,
        scratch_shapes=[
            pltpu.VMEM((count, rows, columns), dtype),
            pltpu.SemaphoreType.DMA((count,)),
            pltpu.SemaphoreType.DMA((count, parts)),
            pltpu.SemaphoreType.DMA((count, 2 * outer - 1)),
            pltpu.SemaphoreType.DMA((count, 2 * outer)),
        ],
        compiler_params=pltpu.CompilerParams(
            collective_id=0, has_side_effects=True, vmem_limit_bytes=8 * 1024 * 1024
        ),
        cost_estimate=pl.CostEstimate(
            flops=200_000_000, bytes_accessed=2 * parts * size, transcendentals=0
        ),
    )(*blocks)
    return [out.reshape(parts * rows, columns) for out in outs]


def scatter_kernel(outer, scale, left, right, out, psend, precv, total, first, second,
                   psend_sem, precv_sem, send1, recv1, send2, recv2):
    count = right.shape[0]
    rows = out.shape[1]
    half = rows // 2
    chips = 2 * outer
    a, b, c = place(outer)
    partner = index_of(a, b, 1 - c)
    across = index_of(a, 1 - b, c)
    greet(outer, a, b, c)

    def spot(p):
        return (p % outer + 1) % outer, 1 - p // outer

    def term(p, w, core, h):
        da, db = spot(p)
        owner = index_of((a + da) % outer, (b + db) % 2, core)
        start = pl.multiple_of(owner * rows + h * half, 16)
        return jnp.dot(
            left[w // 2, pl.ds(start, half), :], right[w], preferred_element_type=jnp.float32
        )

    def part(h):
        return pl.ds(pl.multiple_of(h * half, 16), half)

    def to_partner(p, w):
        return remote(psend.at[p, w], precv.at[p, w], psend_sem.at[p, w], precv_sem.at[p, w], partner)

    def hop1_across(p, w):
        da, _ = spot(p)
        return remote(total.at[p, w], first.at[da, w], send1.at[p, w], recv1.at[da, w], across)

    def hop1_along(p, w):
        da, db = spot(p)
        slot = (da - 1) * 2 + db
        target = index_of((a + da) % outer, b, c)
        return remote(total.at[p, w], first.at[slot, w], send1.at[p, w], recv1.at[slot, w], target)

    def first_arrived(slot, w):
        remote(first.at[slot, w], first.at[slot, w], send1.at[0, w], recv1.at[slot, w],
               across).wait_recv()

    def second_arrived(slot, w):
        remote(second.at[slot, w], second.at[slot, w], send2.at[0, w], recv2.at[slot, w],
               across).wait_recv()

    @pl.loop(0, chips * count)
    def _(i):
        p, w = i // count, i % count

        @pl.loop(0, 2)
        def _(h):
            psend[p, w, part(h), :] = term(p, w, 1 - c, h).astype(psend.dtype)

        to_partner(p, w).start()

    @pl.loop(0, chips * count)
    def _(i):
        p, w = i // count, i % count
        da, db = spot(p)
        to_partner(p, w).wait_recv()

        @pl.loop(0, 2)
        def _(h):
            total[p, w, part(h), :] = (
                term(p, w, c, h) + precv[p, w, part(h), :].astype(jnp.float32)
            ).astype(total.dtype)

        @pl.when((c == 0) & (db == 1))
        def _():
            hop1_across(p, w).start()

        @pl.when((c == 1) & (da != 0))
        def _():
            hop1_along(p, w).start()

    spots = [((p % outer + 1) % outer, 1 - p // outer) for p in range(chips)]
    where = {key: p for p, key in enumerate(spots)}

    def hop2(p, slot, w, target):
        return remote(total.at[p, w], second.at[slot, w], send2.at[slot, w], recv2.at[slot, w], target)

    def hop2_along(da, w):
        return hop2(where[da, 0], da - 1, w, index_of((a + da) % outer, b, c))

    def hop2_across(w):
        return hop2(where[0, 1], 0, w, across)

    def summed(p, w, slots, h):
        value = total[p, w, part(h), :].astype(jnp.float32)
        for ref, slot in slots:
            value = value + ref[slot, w, part(h), :].astype(jnp.float32)
        return value

    def settle(p, w, slots):
        @pl.loop(0, 2)
        def _(h):
            total[p, w, part(h), :] = summed(p, w, slots, h).astype(total.dtype)

    def finish(w, slots):
        @pl.loop(0, 2)
        def _(h):
            out[w, part(h), :] = (summed(where[0, 0], w, slots, h) * scale).astype(out.dtype)

    @pl.when(c == 0)
    def _():
        @pl.loop(0, count)
        def _(w):
            for da in range(1, outer):
                first_arrived(da, w)
                settle(where[da, 0], w, [(first, da)])
                hop2_along(da, w).start()

        @pl.loop(0, count)
        def _(w):
            first_arrived(0, w)
            for da in range(1, outer):
                second_arrived(da - 1, w)
            finish(w, [(first, 0)] + [(second, da - 1) for da in range(1, outer)])
            for da in range(outer):
                hop1_across(where[da, 1], w).wait_send()
            for da in range(1, outer):
                hop2_along(da, w).wait_send()

    @pl.when(c == 1)
    def _():
        @pl.loop(0, count)
        def _(w):
            slots = [(da - 1) * 2 + 1 for da in range(1, outer)]
            for slot in slots:
                first_arrived(slot, w)
            settle(where[0, 1], w, [(first, slot) for slot in slots])
            hop2_across(w).start()

        @pl.loop(0, count)
        def _(w):
            slots = [(da - 1) * 2 for da in range(1, outer)]
            for slot in slots:
                first_arrived(slot, w)
            second_arrived(0, w)
            finish(w, [(first, slot) for slot in slots] + [(second, 0)])
            for da in range(1, outer):
                for db in range(2):
                    hop1_along(where[da, db], w).wait_send()
            hop2_across(w).wait_send()

    @pl.loop(0, chips * count)
    def _(i):
        to_partner(i // count, i % count).wait_send()


def scatter_products(left, right, parts, scale):
    outer, count = parts // 4, right.shape[0]
    rows, columns = left.shape[1] // parts, right.shape[2]
    chips = 2 * outer
    hop1 = max(outer, 2 * (outer - 1))
    hop2 = max(outer - 1, 1)
    block = (count, rows, columns)
    dma = pltpu.SemaphoreType.DMA
    return pl.pallas_call(
        functools.partial(scatter_kernel, outer, scale),
        out_shape=jax.ShapeDtypeStruct(block, jnp.bfloat16),
        in_specs=[pl.BlockSpec(memory_space=pltpu.VMEM)] * 2,
        out_specs=pl.BlockSpec(memory_space=pltpu.VMEM),
        scratch_shapes=[
            pltpu.VMEM((chips,) + block, jnp.bfloat16),
            pltpu.VMEM((chips,) + block, jnp.bfloat16),
            pltpu.VMEM((chips,) + block, jnp.bfloat16),
            pltpu.VMEM((hop1,) + block, jnp.bfloat16),
            pltpu.VMEM((hop2,) + block, jnp.bfloat16),
            dma((chips, count)),
            dma((chips, count)),
            dma((chips, count)),
            dma((hop1, count)),
            dma((hop2, count)),
            dma((hop2, count)),
        ],
        compiler_params=pltpu.CompilerParams(
            collective_id=1, has_side_effects=True, vmem_limit_bytes=VMEM_LIMIT
        ),
        cost_estimate=pl.CostEstimate(
            flops=2 * left.shape[1] * left.shape[2] * columns * count,
            bytes_accessed=2 * chips * count * rows * columns * 2,
            transcendentals=0,
        ),
    )(left, right)


def body(parts, layer_inputs, out_grad, pre_scale, post_scale, gate_weight, up_weight, down_weight):
    tok_rows = out_grad.shape[0]
    layer_count = layer_inputs.shape[0]
    grad_scale = 1.0 / math.sqrt(tok_rows * lax.axis_size("fsdp") * lax.axis_size("tp"))
    carried = out_grad.astype(jnp.float32)
    gate_list = [None] * layer_count
    up_list = [None] * layer_count
    down_list = [None] * layer_count

    def nt(x, y):
        return lax.dot_general(x, y, (((1,), (1,)), ((), ())), preferred_element_type=jnp.float32)

    for layer_id in reversed(range(layer_count)):
        layer_in = layer_inputs[layer_id].astype(jnp.float32)
        first_rms = rms_factor(layer_in)
        normed = (layer_in * first_rms * pre_scale[layer_id]).astype(jnp.bfloat16)
        normed_group = lax.all_gather(normed, "tp", axis=0, tiled=True)
        full_gate, full_up, full_down = gather_blocks(
            [gate_weight[layer_id], up_weight[layer_id], down_weight[layer_id].T], parts
        )
        gate_pre = jnp.dot(normed_group, full_gate, preferred_element_type=jnp.float32)
        up_pre = jnp.dot(normed_group, full_up, preferred_element_type=jnp.float32)
        active, gelu_back = jax.vjp(gelu_tanh, gate_pre)
        hidden = (active * up_pre).astype(jnp.bfloat16)
        partial_mlp = nt(hidden, full_down)
        mlp_out = lax.psum_scatter(
            partial_mlp.astype(jnp.bfloat16), "tp", scatter_dimension=0, tiled=True
        ).astype(jnp.float32)
        mlp_out = lax.optimization_barrier(mlp_out.astype(jnp.bfloat16)).astype(jnp.float32)
        second_rms = rms_factor(mlp_out)
        mlp_grad = norm_back(
            carried * post_scale[layer_id], mlp_out * second_rms, second_rms
        ).astype(jnp.bfloat16)
        grad_group = lax.all_gather(mlp_grad, "tp", axis=0, tiled=True)
        hidden_grad = jnp.dot(grad_group, full_down, preferred_element_type=jnp.float32)
        gate_delta = gelu_back(hidden_grad * up_pre)[0].astype(jnp.bfloat16)
        up_delta = (hidden_grad * active).astype(jnp.bfloat16)
        partial_grad = nt(gate_delta, full_gate) + nt(up_delta, full_up)
        normed_grad = lax.psum_scatter(
            partial_grad.astype(jnp.bfloat16), "tp", scatter_dimension=0, tiled=True
        ).astype(jnp.float32)
        summed = scatter_products(
            jnp.stack([normed_group.T, grad_group.T]),
            jnp.stack([gate_delta, up_delta, hidden]),
            parts,
            grad_scale,
        )
        gate_list[layer_id] = summed[0]
        up_list[layer_id] = summed[1]
        down_list[layer_id] = summed[2].T
        carried = carried + norm_back(
            normed_grad * pre_scale[layer_id], layer_in * first_rms, first_rms
        )
    return (
        carried.astype(jnp.bfloat16),
        jnp.stack(gate_list),
        jnp.stack(up_list),
        jnp.stack(down_list),
    )


def solution(mesh):
    in_specs = (
        P(None, ("fsdp", "tp"), None),
        P(("fsdp", "tp"), None),
        P(),
        P(),
        P(None, "fsdp", "tp"),
        P(None, "fsdp", "tp"),
        P(None, "tp", "fsdp"),
    )
    out_specs = (
        P(("fsdp", "tp"), None),
        P(None, "fsdp", "tp"),
        P(None, "fsdp", "tp"),
        P(None, "tp", "fsdp"),
    )
    step = functools.partial(body, mesh.shape["fsdp"])
    return jax.shard_map(step, mesh=mesh, in_specs=in_specs, out_specs=out_specs, check_vma=False)
```

```python
import functools
import math

import jax
import jax.numpy as jnp
from jax import lax
from jax.experimental import pallas as pl
from jax.experimental.pallas import tpu as pltpu
from jax.sharding import PartitionSpec as P

epsilon = 1e-06
MESH = pl.DeviceIdType.MESH
VMEM_LIMIT = 60 * 1024 * 1024


def rms_factor(values):
    return lax.rsqrt(jnp.mean(values * values, axis=-1, keepdims=True) + epsilon)


def norm_back(delta, normed_in, factor):
    return factor * (delta - normed_in * jnp.mean(delta * normed_in, axis=-1, keepdims=True))


def gelu_tanh(values):
    return jax.nn.gelu(values, approximate=True)


def place(outer):
    me = lax.axis_index("fsdp")
    return me // 4, (me // 2) % 2, me % 2


def index_of(a, b, c):
    return (a * 2 + b) * 2 + c


def remote(src, dst, send_sem, recv_sem, target):
    return pltpu.make_async_remote_copy(
        src_ref=src,
        dst_ref=dst,
        send_sem=send_sem,
        recv_sem=recv_sem,
        device_id={"fsdp": target},
        device_id_type=MESH,
    )


def greet(outer, a, b, c):
    barrier = pltpu.get_barrier_semaphore()
    targets = [index_of(a, b, 1 - c), index_of(a, 1 - b, c)]
    targets += [index_of((a + j) % outer, b, c) for j in range(1, outer)]
    for target in targets:
        pl.semaphore_signal(barrier, inc=1, device_id={"fsdp": target}, device_id_type=MESH)
    pl.semaphore_wait(barrier, len(targets))


def gather_kernel(outer, count, *refs):
    ins, outs = refs[:count], refs[count : 2 * count]
    bounce, local_sem, recv_sem, link_sem, pair_sem = refs[2 * count :]
    a, b, c = place(outer)
    me = index_of(a, b, c)
    partner = index_of(a, b, 1 - c)
    across = index_of(a, 1 - b, c)
    along = [index_of((a + j) % outer, b, c) for j in range(1, outer)]
    diagonal = [index_of((a + j) % outer, 1 - b, c) for j in range(1, outer)]
    greet(outer, a, b, c)

    def push(w, src, slot, sem, target):
        return remote(src, outs[w].at[slot], sem, recv_sem.at[w, slot], target)

    def arrived(w, slot):
        spot = outs[w].at[slot]
        remote(spot, spot, pair_sem.at[w, 0], recv_sem.at[w, slot], partner).wait_recv()

    sent = []
    for w in range(count):
        own = [push(w, ins[w], me, link_sem.at[w, 0], across)]
        own += [push(w, ins[w], me, link_sem.at[w, 1 + j], t) for j, t in enumerate(along)]
        own.append(push(w, ins[w], me, pair_sem.at[w, 0], partner))
        for copy in own:
            copy.start()
        sent += own
    inward = [pltpu.make_async_copy(ins[w], bounce.at[w], local_sem.at[w]) for w in range(count)]
    outward = [
        pltpu.make_async_copy(bounce.at[w], outs[w].at[me], local_sem.at[w]) for w in range(count)
    ]
    for w in range(count):
        inward[w].start()
    for w in range(count):
        inward[w].wait()
        outward[w].start()
    forwards = []
    for w in range(count):
        arrived(w, across)
        copy = push(w, outs[w].at[across], across, pair_sem.at[w, 1], partner)
        copy.start()
        sent.append(copy)
        for j, target in enumerate(along):
            copy = push(w, outs[w].at[across], across, link_sem.at[w, outer + j], target)
            pl.when(c == 0)(copy.start)
            forwards.append((0, copy))
        for j, slot in enumerate(along):
            arrived(w, slot)
            copy = push(w, outs[w].at[slot], slot, link_sem.at[w, outer + j], across)
            pl.when(c == 1)(copy.start)
            forwards.append((1, copy))
            copy = push(w, outs[w].at[slot], slot, pair_sem.at[w, 2 + j], partner)
            copy.start()
            sent.append(copy)
    for w in range(count):
        for j, slot in enumerate(diagonal):
            arrived(w, slot)
            copy = push(w, outs[w].at[slot], slot, pair_sem.at[w, 1 + outer + j], partner)
            copy.start()
            sent.append(copy)
    for w in range(count):
        for chip in range(2 * outer):
            arrived(w, chip * 2 + 1 - c)
        outward[w].wait()
    for copy in sent:
        copy.wait_send()
    for core, copy in forwards:
        pl.when(c == core)(copy.wait_send)


def gather_blocks(blocks, parts):
    outer, count = parts // 4, len(blocks)
    rows, columns = blocks[0].shape
    dtype = blocks[0].dtype
    size = rows * columns * dtype.itemsize * count
    outs = pl.pallas_call(
        functools.partial(gather_kernel, outer, count),
        out_shape=[jax.ShapeDtypeStruct((parts, rows, columns), dtype)] * count,
        in_specs=[pl.BlockSpec(memory_space=pl.ANY)] * count,
        out_specs=[pl.BlockSpec(memory_space=pl.ANY)] * count,
        scratch_shapes=[
            pltpu.VMEM((count, rows, columns), dtype),
            pltpu.SemaphoreType.DMA((count,)),
            pltpu.SemaphoreType.DMA((count, parts)),
            pltpu.SemaphoreType.DMA((count, 2 * outer - 1)),
            pltpu.SemaphoreType.DMA((count, 2 * outer)),
        ],
        compiler_params=pltpu.CompilerParams(
            collective_id=0, has_side_effects=True, vmem_limit_bytes=VMEM_LIMIT
        ),
        cost_estimate=pl.CostEstimate(
            flops=200_000_000, bytes_accessed=2 * parts * size, transcendentals=0
        ),
    )(*blocks)
    return [out.reshape(parts * rows, columns) for out in outs]


def scatter_kernel(outer, scale, left, right, out, psend, precv, total, first, second,
                   psend_sem, precv_sem, send1, recv1, send2, recv2):
    count = right.shape[0]
    rows = out.shape[1]
    half = rows // 2
    chips = 2 * outer
    a, b, c = place(outer)
    partner = index_of(a, b, 1 - c)
    across = index_of(a, 1 - b, c)
    greet(outer, a, b, c)

    def spot(p):
        return (p % outer + 1) % outer, 1 - p // outer

    def term(p, w, core, h):
        da, db = spot(p)
        owner = index_of((a + da) % outer, (b + db) % 2, core)
        start = pl.multiple_of(owner * rows + h * half, 16)
        return jnp.dot(
            left[w // 2, pl.ds(start, half), :], right[w], preferred_element_type=jnp.float32
        )

    def part(h):
        return pl.ds(pl.multiple_of(h * half, 16), half)

    def to_partner(p, w):
        return remote(psend.at[p, w], precv.at[p, w], psend_sem.at[p, w], precv_sem.at[p, w], partner)

    def hop1_across(p, w):
        da, _ = spot(p)
        return remote(total.at[p, w], first.at[da, w], send1.at[p, w], recv1.at[da, w], across)

    def hop1_along(p, w):
        da, db = spot(p)
        slot = (da - 1) * 2 + db
        target = index_of((a + da) % outer, b, c)
        return remote(total.at[p, w], first.at[slot, w], send1.at[p, w], recv1.at[slot, w], target)

    def first_arrived(slot, w):
        remote(first.at[slot, w], first.at[slot, w], send1.at[0, w], recv1.at[slot, w],
               across).wait_recv()

    def second_arrived(slot, w):
        remote(second.at[slot, w], second.at[slot, w], send2.at[0, w], recv2.at[slot, w],
               across).wait_recv()

    @pl.loop(0, chips * count)
    def _(i):
        p, w = i // count, i % count

        @pl.loop(0, 2)
        def _(h):
            psend[p, w, part(h), :] = term(p, w, 1 - c, h).astype(psend.dtype)

        to_partner(p, w).start()

    @pl.loop(0, chips * count)
    def _(i):
        p, w = i // count, i % count
        da, db = spot(p)
        to_partner(p, w).wait_recv()

        @pl.loop(0, 2)
        def _(h):
            total[p, w, part(h), :] = (
                term(p, w, c, h) + precv[p, w, part(h), :].astype(jnp.float32)
            ).astype(total.dtype)

        @pl.when((c == 0) & (db == 1))
        def _():
            hop1_across(p, w).start()

        @pl.when((c == 1) & (da != 0))
        def _():
            hop1_along(p, w).start()

    spots = [((p % outer + 1) % outer, 1 - p // outer) for p in range(chips)]
    where = {key: p for p, key in enumerate(spots)}

    def hop2(p, slot, w, target):
        return remote(total.at[p, w], second.at[slot, w], send2.at[slot, w], recv2.at[slot, w], target)

    def hop2_along(da, w):
        return hop2(where[da, 0], da - 1, w, index_of((a + da) % outer, b, c))

    def hop2_across(w):
        return hop2(where[0, 1], 0, w, across)

    def summed(p, w, slots, h):
        value = total[p, w, part(h), :].astype(jnp.float32)
        for ref, slot in slots:
            value = value + ref[slot, w, part(h), :].astype(jnp.float32)
        return value

    def settle(p, w, slots):
        @pl.loop(0, 2)
        def _(h):
            total[p, w, part(h), :] = summed(p, w, slots, h).astype(total.dtype)

    def finish(w, slots):
        @pl.loop(0, 2)
        def _(h):
            out[w, part(h), :] = (summed(where[0, 0], w, slots, h) * scale).astype(out.dtype)

    @pl.when(c == 0)
    def _():
        @pl.loop(0, count)
        def _(w):
            for da in range(1, outer):
                first_arrived(da, w)
                settle(where[da, 0], w, [(first, da)])
                hop2_along(da, w).start()

        @pl.loop(0, count)
        def _(w):
            first_arrived(0, w)
            for da in range(1, outer):
                second_arrived(da - 1, w)
            finish(w, [(first, 0)] + [(second, da - 1) for da in range(1, outer)])
            for da in range(outer):
                hop1_across(where[da, 1], w).wait_send()
            for da in range(1, outer):
                hop2_along(da, w).wait_send()

    @pl.when(c == 1)
    def _():
        @pl.loop(0, count)
        def _(w):
            slots = [(da - 1) * 2 + 1 for da in range(1, outer)]
            for slot in slots:
                first_arrived(slot, w)
            settle(where[0, 1], w, [(first, slot) for slot in slots])
            hop2_across(w).start()

        @pl.loop(0, count)
        def _(w):
            slots = [(da - 1) * 2 for da in range(1, outer)]
            for slot in slots:
                first_arrived(slot, w)
            second_arrived(0, w)
            finish(w, [(first, slot) for slot in slots] + [(second, 0)])
            for da in range(1, outer):
                for db in range(2):
                    hop1_along(where[da, db], w).wait_send()
            hop2_across(w).wait_send()

    @pl.loop(0, chips * count)
    def _(i):
        to_partner(i // count, i % count).wait_send()


def scatter_products(left, right, parts, scale):
    outer, count = parts // 4, right.shape[0]
    rows, columns = left.shape[1] // parts, right.shape[2]
    chips = 2 * outer
    hop1 = max(outer, 2 * (outer - 1))
    hop2 = max(outer - 1, 1)
    block = (count, rows, columns)
    dma = pltpu.SemaphoreType.DMA
    return pl.pallas_call(
        functools.partial(scatter_kernel, outer, scale),
        out_shape=jax.ShapeDtypeStruct(block, jnp.bfloat16),
        in_specs=[pl.BlockSpec(memory_space=pltpu.VMEM)] * 2,
        out_specs=pl.BlockSpec(memory_space=pltpu.VMEM),
        scratch_shapes=[
            pltpu.VMEM((chips,) + block, jnp.bfloat16),
            pltpu.VMEM((chips,) + block, jnp.bfloat16),
            pltpu.VMEM((chips,) + block, jnp.bfloat16),
            pltpu.VMEM((hop1,) + block, jnp.bfloat16),
            pltpu.VMEM((hop2,) + block, jnp.bfloat16),
            dma((chips, count)),
            dma((chips, count)),
            dma((chips, count)),
            dma((hop1, count)),
            dma((hop2, count)),
            dma((hop2, count)),
        ],
        compiler_params=pltpu.CompilerParams(
            collective_id=1, has_side_effects=True, vmem_limit_bytes=VMEM_LIMIT
        ),
        cost_estimate=pl.CostEstimate(
            flops=2 * left.shape[1] * left.shape[2] * columns * count,
            bytes_accessed=2 * chips * count * rows * columns * 2,
            transcendentals=0,
        ),
    )(left, right)


def middle_kernel(span, chunks, partial, carried, post, out, from_left, from_right,
                  right_send, right_recv, left_send, left_recv,
                  gather_right, gather_left, gather_recv):
    t = lax.axis_index("tp")
    rows, width = carried.shape
    piece = rows // chunks
    last = span - 1

    def hop(src, dst, send_sem, recv_sem, target):
        return pltpu.make_async_remote_copy(
            src_ref=src,
            dst_ref=dst,
            send_sem=send_sem,
            recv_sem=recv_sem,
            device_id={"tp": target},
            device_id_type=MESH,
        )

    def right_hop(k, o):
        spot = from_left.at[k, o]
        return hop(spot, spot, right_send.at[k, o], right_recv.at[k, o], t + 1)

    def left_hop(k, o):
        spot = from_right.at[k, o]
        return hop(spot, spot, left_send.at[k, o], left_recv.at[k, o], t - 1)

    def block(o, k):
        return pl.ds(pl.multiple_of(o * rows + k * piece, 16), piece)

    def gather_hop(k, o, sem, target):
        spot = out.at[block(o, k)]
        return hop(spot, spot, sem, gather_recv.at[k, o], target)

    barrier = pltpu.get_barrier_semaphore()

    @pl.when(t > 0)
    def _():
        pl.semaphore_signal(barrier, inc=1, device_id={"tp": t - 1}, device_id_type=MESH)

    @pl.when(t < last)
    def _():
        pl.semaphore_signal(barrier, inc=1, device_id={"tp": t + 1}, device_id_type=MESH)

    @pl.when((t > 0) & (t < last))
    def _():
        pl.semaphore_wait(barrier, 2)

    @pl.when((t == 0) | (t == last))
    def _():
        pl.semaphore_wait(barrier, 1)

    def add_into(ref, k, o):
        ref[k, o] = (
            ref[k, o].astype(jnp.float32) + partial[block(o, k), :].astype(jnp.float32)
        ).astype(ref.dtype)

    def pass_on(k):
        for i in range(last):
            o = last - i

            @pl.when(t == 0)
            def _():
                from_left[k, o] = partial[block(o, k), :]
                right_hop(k, o).start()

            @pl.when((t > 0) & (t < o))
            def _():
                right_hop(k, o).wait_recv()
                add_into(from_left, k, o)
                right_hop(k, o).start()

            @pl.when(t == last)
            def _():
                from_right[k, i] = partial[block(i, k), :]
                left_hop(k, i).start()

            @pl.when((t < last) & (t > i))
            def _():
                left_hop(k, i).wait_recv()
                add_into(from_right, k, i)
                left_hop(k, i).start()

    def settle(k):
        @pl.when(t > 0)
        def _():
            right_hop(k, t).wait_recv()

        @pl.when(t == 0)
        def _():
            from_left[k, 0] = jnp.zeros_like(from_left[k, 0])

        @pl.when(t < last)
        def _():
            left_hop(k, t).wait_recv()

        @pl.when(t == last)
        def _():
            from_right[k, last] = jnp.zeros_like(from_right[k, last])

        whole = partial[block(t, k), :].astype(jnp.float32)
        whole = whole + from_left[k, t].astype(jnp.float32)
        whole = whole + from_right[k, t].astype(jnp.float32)
        whole = whole.astype(jnp.bfloat16).astype(jnp.float32)
        factor = rms_factor(whole)
        delta = carried[pl.ds(k * piece, piece), :] * post[...]
        out[block(t, k), :] = norm_back(delta, whole * factor, factor).astype(out.dtype)

        @pl.when(t < last)
        def _():
            gather_hop(k, t, gather_right.at[k, t], t + 1).start()

        @pl.when(t > 0)
        def _():
            gather_hop(k, t, gather_left.at[k, t], t - 1).start()

    def spread(k):
        for i in range(span):
            o = last - i

            @pl.when(o < t)
            def _():
                gather_hop(k, o, gather_right.at[k, o], t - 1).wait_recv()

                @pl.when(t < last)
                def _():
                    gather_hop(k, o, gather_right.at[k, o], t + 1).start()

            @pl.when(i > t)
            def _():
                gather_hop(k, i, gather_left.at[k, i], t + 1).wait_recv()

                @pl.when(t > 0)
                def _():
                    gather_hop(k, i, gather_left.at[k, i], t - 1).start()

    for step in range(chunks + 2):
        if step < chunks:
            pass_on(step)
        if 0 <= step - 1 < chunks:
            settle(step - 1)
        if 0 <= step - 2:
            spread(step - 2)
    for k in range(chunks):
        for o in range(span):

            @pl.when(t < o)
            def _():
                right_hop(k, o).wait_send()

            @pl.when(t > o)
            def _():
                left_hop(k, o).wait_send()

            @pl.when((o <= t) & (t < last))
            def _():
                gather_hop(k, o, gather_right.at[k, o], t + 1).wait_send()

            @pl.when((o >= t) & (t > 0))
            def _():
                gather_hop(k, o, gather_left.at[k, o], t - 1).wait_send()


def middle_exchange(partial, carried, post, span):
    rows, width = carried.shape
    chunks = 4 if rows % 64 == 0 else 1
    slots = pltpu.VMEM((chunks, span, rows // chunks, width), jnp.bfloat16)
    return pl.pallas_call(
        functools.partial(middle_kernel, span, chunks),
        out_shape=jax.ShapeDtypeStruct(partial.shape, jnp.bfloat16),
        in_specs=[pl.BlockSpec(memory_space=pltpu.VMEM)] * 3,
        out_specs=pl.BlockSpec(memory_space=pltpu.VMEM),
        scratch_shapes=[slots, slots] + [pltpu.SemaphoreType.DMA((chunks, span))] * 7,
        compiler_params=pltpu.CompilerParams(
            collective_id=2, has_side_effects=True, vmem_limit_bytes=32 * 1024 * 1024
        ),
        cost_estimate=pl.CostEstimate(
            flops=200_000_000, bytes_accessed=4 * partial.size, transcendentals=0
        ),
    )(partial, carried, post)


def body(parts, layer_inputs, out_grad, pre_scale, post_scale, gate_weight, up_weight, down_weight):
    tok_rows = out_grad.shape[0]
    layer_count = layer_inputs.shape[0]
    grad_scale = 1.0 / math.sqrt(tok_rows * lax.axis_size("fsdp") * lax.axis_size("tp"))
    carried = out_grad.astype(jnp.float32)
    gate_list = [None] * layer_count
    up_list = [None] * layer_count
    down_list = [None] * layer_count

    def nt(x, y):
        return lax.dot_general(x, y, (((1,), (1,)), ((), ())), preferred_element_type=jnp.float32)

    for layer_id in reversed(range(layer_count)):
        layer_in = layer_inputs[layer_id].astype(jnp.float32)
        first_rms = rms_factor(layer_in)
        normed = (layer_in * first_rms * pre_scale[layer_id]).astype(jnp.bfloat16)
        normed_group = lax.all_gather(normed, "tp", axis=0, tiled=True)
        full_gate, full_up, full_down = gather_blocks(
            [gate_weight[layer_id], up_weight[layer_id], down_weight[layer_id].T], parts
        )
        gate_pre = jnp.dot(normed_group, full_gate, preferred_element_type=jnp.float32)
        up_pre = jnp.dot(normed_group, full_up, preferred_element_type=jnp.float32)
        active, gelu_back = jax.vjp(gelu_tanh, gate_pre)
        hidden = (active * up_pre).astype(jnp.bfloat16)
        partial_mlp = nt(hidden, full_down)
        grad_group = middle_exchange(
            partial_mlp.astype(jnp.bfloat16),
            carried,
            post_scale[layer_id][None],
            lax.axis_size("tp"),
        )
        hidden_grad = jnp.dot(grad_group, full_down, preferred_element_type=jnp.float32)
        gate_delta = gelu_back(hidden_grad * up_pre)[0].astype(jnp.bfloat16)
        up_delta = (hidden_grad * active).astype(jnp.bfloat16)
        partial_grad = nt(gate_delta, full_gate) + nt(up_delta, full_up)
        normed_grad = lax.psum_scatter(
            partial_grad.astype(jnp.bfloat16), "tp", scatter_dimension=0, tiled=True
        ).astype(jnp.float32)
        summed = scatter_products(
            jnp.stack([normed_group.T, grad_group.T]),
            jnp.stack([gate_delta, up_delta, hidden]),
            parts,
            grad_scale,
        )
        gate_list[layer_id] = summed[0]
        up_list[layer_id] = summed[1]
        down_list[layer_id] = summed[2].T
        carried = carried + norm_back(
            normed_grad * pre_scale[layer_id], layer_in * first_rms, first_rms
        )
    return (
        carried.astype(jnp.bfloat16),
        jnp.stack(gate_list),
        jnp.stack(up_list),
        jnp.stack(down_list),
    )


def solution(mesh):
    in_specs = (
        P(None, ("fsdp", "tp"), None),
        P(("fsdp", "tp"), None),
        P(),
        P(),
        P(None, "fsdp", "tp"),
        P(None, "fsdp", "tp"),
        P(None, "tp", "fsdp"),
    )
    out_specs = (
        P(("fsdp", "tp"), None),
        P(None, "fsdp", "tp"),
        P(None, "fsdp", "tp"),
        P(None, "tp", "fsdp"),
    )
    step = functools.partial(body, mesh.shape["fsdp"])
    return jax.shard_map(step, mesh=mesh, in_specs=in_specs, out_specs=out_specs, check_vma=False)
```
